32 devices in a mesh: grp: 2 (over x), slab: 16 (over z, y, core).
Axes of the slice: x: 2, y: 2, z: 4, core: 2. Of those that a mesh axis runs over, the one named last changes fastest.
Arguments:
- volume: bfloat16 [64, 1024, 1024], P(('grp', 'slab')), parts along dimension 0, may hold values from -60 to 60
- plane_shift: int32 [4, 32], P('grp', 'slab'), parts along dimension 0, may hold values from -64 to 64
- plane_weight: float32 [4, 32], P('grp', 'slab'), parts along dimension 0, may hold values from 0 to 1
- column_left: int32 [4, 1024], P('grp'), parts along dimension 0, may hold values from 0 to 1022
- column_weight: float32 [4, 1024], P('grp'), parts along dimension 0, may hold values from 0 to 1
- window_center: int32 [4, 2], P('grp'), parts along dimension 0, may hold values from -200 to 199
- tilt_owner: int32 [32], P('grp'), parts along dimension 0, may hold values from 0 to 15, each once
- reference_band: float32 [32, 2, 128, 128], P(('grp', 'slab')), parts along dimension 0, may hold values from -6 to 6
Outputs:
- correlation: float32 [4, 16, 128], P('grp', 'slab'), parts along dimension 0
- peaks: float32 [4], P('grp'), parts along dimension 0
The draws below stay inside these ranges and needn't reach their ends.
There are 2 independent parts, one for each index of `grp`. The reference program is written for one: setup_inputs(seed, part) draws one part's arguments, and reference() takes and returns one part's arrays. A program takes and returns all parts, laid end to end along the dimension named above; each array names one. Nothing has to cross between parts.
Inputs may be any that keep to these rules, and one draw needn't show every extreme that they name: `tilt_owner`: the first 2 entries name the owners of the tilts, one slab index each.
All inputs are finite; a program needn't handle non-finite values.
Results may differ from the reference program's by a relative error of at most 0.0003.
Values sent between devices are 32-bit elements; how exact they have to be, the bound alone decides.
A program may use at most 128 MiB of HBM per device.

```python
import math
import jax
import jax.numpy as jnp
from jax import lax

Y = 1024
X = 1024
BAND = 128
WIN_COLS = 128
TILTS = 2
PLANES = 32
WIN_ROWS = 16
N_SLAB = 16


def draw_volume(key, part):
    first_key, second_key, third_key = jax.random.split(key, 3)
    col_scale = jnp.exp(jax.random.uniform(second_key, (1, 1, X), jnp.float32) * math.log(10.0))
    row_scale = jnp.exp(jax.random.uniform(third_key, (1, Y, 1), jnp.float32) * math.log(10.0))
    base = jnp.clip(jax.random.normal(first_key, (PLANES, Y, X), jnp.float32), -6.0, 6.0)
    return (base * col_scale * row_scale / 10.0).astype(jnp.bfloat16)


def set_ends(values, own_key, smallest, high):
    dims = values.shape
    place = [jax.random.randint(jax.random.fold_in(own_key, axis), (), 0, dims[axis]) for axis in range(len(dims))]
    values = values.at[tuple(place)].set(smallest)
    longest = dims.index(max(dims))
    place[longest] = (place[longest] + 1) % dims[longest]
    return values.at[tuple(place)].set(high)


def level_of(key, extent, pieces, least, largest):
    factor_of = 1.0
    for dim, shards_of in pieces:
        draws = jax.random.uniform(jax.random.fold_in(jax.random.fold_in(key, 6), dim), (shards_of,), jnp.float32, least / len(pieces), largest / len(pieces))
        factor_of = factor_of * jnp.repeat(jnp.exp(draws), extent[dim] // shards_of).reshape((-1,) + (1,) * (len(extent) - 1 - dim))
    return factor_of


def gaussian(own_key, extent, spread, most, cuts=(), kind=jnp.bfloat16):
    result = jax.random.normal(own_key, extent, jnp.float32) * spread
    if len(cuts) > 0:
        result = level_of(own_key, extent, cuts, -0.22, 0.18) * result
    return jnp.clip(result, min=-most, max=most).astype(kind)


def setup_inputs(seed: int = 0, part: int = 0) -> dict:
    seeds = jax.random.split(jax.random.key(seed), 9)
    own_keys = jax.random.split(jax.random.fold_in(seeds[8], part), 9)
    volume = draw_volume(jax.random.fold_in(jax.random.fold_in(seeds[8], part), 71), part)
    plane_shift = set_ends(jax.random.randint(own_keys[1], (TILTS, PLANES), -(X // 16), X // 16 + 1), jax.random.fold_in(own_keys[1], 1), -(X // 16), (X // 16 + 1) - 1).astype(jnp.int32)
    plane_weight = jnp.clip(1.0 * jax.random.uniform(own_keys[2], (TILTS, PLANES), jnp.float32) ** level_of(own_keys[2], (TILTS, PLANES), ((1, 16),), -0.2, 0.2), 0.0, 1.0)
    column_left = set_ends(jax.random.randint(own_keys[3], (TILTS, X), 0, X - 1), jax.random.fold_in(own_keys[3], 1), 0, (X - 1) - 1).astype(jnp.int32)
    column_weight = jnp.clip(jax.random.uniform(own_keys[4], (TILTS, X), jnp.float32, 0.0, 1.0), 0.0, 1.0)
    window_center = set_ends(jax.random.randint(own_keys[5], (TILTS, 2), -200, 200), jax.random.fold_in(own_keys[5], 1), -200, 199).astype(jnp.int32)
    tilt_owner = jax.random.permutation(own_keys[6], N_SLAB).astype(jnp.int32)
    reference_band = gaussian(own_keys[7], (N_SLAB, 2, BAND, BAND), 1.0, 6.0, ((0, 16),), jnp.float32)
    return {"volume": volume, "plane_shift": plane_shift, "plane_weight": plane_weight, "column_left": column_left, "column_weight": column_weight, "window_center": window_center, "tilt_owner": tilt_owner, "reference_band": reference_band}


def project_tilt(volume, shift_row, weight_row, left_row, share_row):
    margin = X // 16 + 1

    def add_plane(total, items):
        plane_data, shift_value, weight_value = items
        padded = jnp.pad(plane_data.astype(jnp.float32), ((0, 0), (margin, margin)))
        near_cells = lax.dynamic_slice_in_dim(padded, (margin - shift_value).astype(jnp.int32), X, 1)
        far_cells = lax.dynamic_slice_in_dim(padded, (margin - shift_value - 1).astype(jnp.int32), X, 1)
        return (total + (1.0 - weight_value) * near_cells + weight_value * far_cells, None)
    summed, _ = lax.scan(add_plane, jnp.zeros((Y, X), jnp.float32), (volume, shift_row, weight_row))
    left_values = jnp.take(summed, left_row, axis=1)
    right_values = jnp.take(summed, left_row + 1, axis=1)
    return (1.0 - share_row) * left_values + share_row * right_values

def phase_pair(left_ints, right_ints, length):
    product = left_ints[:, None] * right_ints[None, :] % length
    angle = product.astype(jnp.float32) * (2.0 * math.pi / length)
    return (jnp.cos(angle), jnp.sin(angle))

def matmul(first, second):
    return jnp.dot(first, second, precision=lax.Precision.HIGHEST, preferred_element_type=jnp.float32)

def reference(volume, plane_shift, plane_weight, column_left, column_weight, window_center, tilt_owner, reference_band):
    freq_cols = jnp.arange(BAND, dtype=jnp.int32)
    freq_rows = freq_cols - BAND // 2
    band_rows = freq_rows % Y
    outputs = []
    maxima = []
    for which in range(TILTS):
        projected = project_tilt(volume, plane_shift[which], plane_weight[which], column_left[which], column_weight[which])
        full_spec = jnp.fft.fft2(projected)
        band_spec = jnp.take(full_spec, band_rows, axis=0)[:, :BAND]
        spec_real = jnp.real(band_spec).astype(jnp.float32)
        spec_imag = jnp.imag(band_spec).astype(jnp.float32)
        owned = reference_band[tilt_owner[which]]
        ref_real, ref_imag = (owned[0], owned[1])
        cross_real = spec_real * ref_real + spec_imag * ref_imag
        cross_imag = spec_imag * ref_real - spec_real * ref_imag
        energy_spec = jnp.mean(spec_real * spec_real + spec_imag * spec_imag) + 1e-06
        energy_ref = jnp.mean(ref_real * ref_real + ref_imag * ref_imag) + 1e-06
        offsets_y = window_center[which, 0] + jnp.arange(WIN_ROWS, dtype=jnp.int32) - WIN_ROWS // 2
        offsets_x = window_center[which, 1] + jnp.arange(WIN_COLS, dtype=jnp.int32) - WIN_COLS // 2
        row_cos, row_sin = phase_pair(offsets_y, freq_rows, Y)
        col_cos, col_sin = phase_pair(freq_cols, offsets_x, X)
        half_real = matmul(row_cos, cross_real) - matmul(row_sin, cross_imag)
        half_imag = matmul(row_cos, cross_imag) + matmul(row_sin, cross_real)
        corr = (matmul(half_real, col_cos) - matmul(half_imag, col_sin)) / (BAND * jnp.sqrt(energy_spec * energy_ref))
        outputs.append(corr)
        maxima.append(jnp.max(corr))
    return (jnp.stack(outputs), jnp.stack(maxima))
```

```python
import functools
import math

import jax
import jax.numpy as jnp
import numpy as np
from jax import lax
from jax.experimental import pallas as pl
from jax.experimental.pallas import tpu as pltpu
from jax.sharding import PartitionSpec as P

MESH = pl.DeviceIdType.MESH
LANES = 128
CHUNK = 256
BF16 = jnp.bfloat16
F32 = jnp.float32


def phases(left, right, length):
    angle = (np.outer(left, right) % length) * (2.0 * math.pi / length)
    return np.cos(angle), np.sin(angle)


def split(values):
    high = values.astype(np.float32).astype(BF16)
    low = (values - high.astype(np.float64)).astype(np.float32).astype(BF16)
    return high, low


def halves(value):
    high = value.astype(BF16)
    return high, (value - high.astype(F32)).astype(BF16)


def row_table(length, band):
    count = band // 2 + 8
    cos, sin = phases(np.arange(count), np.arange(length), length)
    return np.concatenate(split(np.concatenate([cos, sin])))


def col_table(length, band):
    cos, sin = phases(np.arange(length), np.arange(band), length)
    return np.stack(split(np.concatenate([cos, sin], axis=1)))


def window_table(length, band, columns):
    cos, sin = phases(np.arange(band), np.arange(columns), length)
    return np.concatenate([cos, sin], axis=1).astype(np.float32)


def partial_kernel(
    shift_ref, weight_ref, left_ref, share_ref, volume_ref, rowt_ref, colt_ref, out_ref,
    vol, rowt, colt, onehot, rows, rolled, summed, stack, proj, sems,
):
    planes, height, width = volume_ref.shape
    tilts = left_ref.shape[0]
    blocks = width // LANES
    chunks = width // CHUNK
    count = rows.shape[2]

    table = pltpu.make_async_copy(rowt_ref, rowt, sems.at[0])
    table.start()
    loads = []
    for z in range(planes):
        for c in range(chunks):
            part = (z, slice(None), pl.ds(c * CHUNK, CHUNK))
            load = pltpu.make_async_copy(volume_ref.at[part], vol.at[part], sems.at[2 + z * chunks + c])
            load.start()
            loads.append(load)
    last_table = pltpu.make_async_copy(colt_ref, colt, sems.at[1])
    last_table.start()

    @pl.loop(0, blocks)
    def _(b):
        first = pl.multiple_of(b * LANES, LANES)
        ids = lax.broadcasted_iota(jnp.int32, (LANES, width), 0) + first
        for t in range(tilts):
            hit = jnp.where(ids == left_ref[t : t + 1, :], 1.0, 0.0)
            onehot[t, pl.ds(first, LANES), :] = hit.astype(BF16)

    table.wait()
    for z in range(planes):
        for c in range(chunks):
            loads[z * chunks + c].wait()
            out = jnp.dot(
                rowt[...], vol[z, :, c * CHUNK : (c + 1) * CHUNK], preferred_element_type=F32
            )
            out = out[:count] + out[count:]
            for b in range(CHUNK // LANES):
                rows[z, c * (CHUNK // LANES) + b] = out[:, b * LANES : (b + 1) * LANES]

    lane = lax.broadcasted_iota(jnp.int32, (count, LANES), 1)
    zero = jnp.zeros((count, LANES), F32)
    for t in range(tilts):
        terms = []
        for z in range(planes):
            for extra in range(2):
                slot = z * 2 + extra
                shift = shift_ref[t, z] + extra
                turn = shift & (LANES - 1)
                jump = jnp.where(shift < 0, 1, 0)
                weight = weight_ref[t, z] if extra else 1.0 - weight_ref[t, z]
                rolled[slot, 0] = zero
                rolled[slot, blocks + 1] = zero
                for b in range(blocks):
                    rolled[slot, b + 1] = pltpu.roll(rows[z, b] * weight, turn, 1)
                terms.append((slot, lane >= turn, jump))
        for b in range(blocks):
            total = None
            for slot, mask, jump in terms:
                term = jnp.where(mask, rolled[slot, b + 1 + jump], rolled[slot, b + jump])
                total = term if total is None else total + term
            summed[b] = total
            high, low = halves(total)
            here = slice(b * LANES, (b + 1) * LANES)
            stack[0, :, here] = high
            stack[1, :, here] = low
        for b in range(blocks):
            ahead = summed[(b + 1) % blocks]
            right = pltpu.roll(jnp.where(lane == 0, ahead, summed[b]), LANES - 1, 1)
            high, low = halves(right)
            here = slice(b * LANES, (b + 1) * LANES)
            stack[2, :, here] = high
            stack[3, :, here] = low
        for c in range(chunks):
            here = slice(c * CHUNK, (c + 1) * CHUNK)
            picked = jnp.dot(
                stack[...].reshape(4 * count, width), onehot[t, :, here], preferred_element_type=F32
            )
            share = share_ref[t : t + 1, here]
            value = (1.0 - share) * (picked[:count] + picked[count : 2 * count])
            value = value + share * (picked[2 * count : 3 * count] + picked[3 * count :])
            high, low = halves(value)
            proj[0, :, here] = high
            proj[1, :, here] = low
        if t == 0:
            last_table.wait()
        both = jnp.dot(
            proj[...].reshape(2 * count, width), colt[0], preferred_element_type=F32
        )
        rest = jnp.dot(proj[0], colt[1], preferred_element_type=F32)
        out_ref[t] = both[:count] + both[count:] + rest


def partial_spectra(shift, weight, left, share, volume, band):
    planes, height, width = volume.shape
    tilts = left.shape[0]
    rowt = row_table(height, band)
    colt = col_table(width, band)
    count = rowt.shape[0] // 2
    blocks = width // LANES
    smem = pl.BlockSpec(memory_space=pltpu.SMEM)
    vmem = pl.BlockSpec(memory_space=pltpu.VMEM)
    hbm = pl.BlockSpec(memory_space=pl.ANY)
    return pl.pallas_call(
        partial_kernel,
        out_shape=jax.ShapeDtypeStruct((tilts, count, 2 * band), F32),
        in_specs=[smem, smem, vmem, vmem, hbm, hbm, hbm],
        out_specs=vmem,
        scratch_shapes=[
            pltpu.VMEM((planes, height, width), BF16),
            pltpu.VMEM(rowt.shape, BF16),
            pltpu.VMEM(colt.shape, BF16),
            pltpu.VMEM((tilts, width, width), BF16),
            pltpu.VMEM((planes, blocks, count, LANES), F32),
            pltpu.VMEM((planes * 2, blocks + 2, count, LANES), F32),
            pltpu.VMEM((blocks, count, LANES), F32),
            pltpu.VMEM((4, count, width), BF16),
            pltpu.VMEM((2, count, width), BF16),
            pltpu.SemaphoreType.DMA((2 + planes * (width // CHUNK),)),
        ],
        compiler_params=pltpu.CompilerParams(vmem_limit_bytes=56 * 1024 * 1024),
        name="partial_spectra",
    )(shift, weight, left, share, volume, jnp.asarray(rowt), jnp.asarray(colt))


def exchange_kernel(
    n, length, center_ref, owner_ref, partial_ref, mine_ref, window_ref, corr_ref, peak_ref,
    ref_out, ref_in, spec_out, spec_in, part_out, part_in, total_ref,
    ref_send, ref_recv, spec_send, spec_recv, part_send, part_recv,
):
    me = lax.axis_index("slab")
    tilts, count, _ = partial_ref.shape
    band = mine_ref.shape[-1]
    half = band // 2
    sines = count // 2
    per = max(1, half // n)
    owners = half // per
    win_cols = corr_ref.shape[-1]

    def on_owner(device, body):
        if owners == n:
            body()
        else:
            pl.when(device < owners)(body)

    barrier = pltpu.get_barrier_semaphore()
    for k in range(1, n):
        pl.semaphore_signal(
            barrier, inc=1, device_id={"slab": lax.rem(me + k, n)}, device_id_type=MESH
        )

    for e in range(owners):
        for part in range(2):
            base = part * 2 * per
            first = half + e * per
            ref_out[e, base : base + per, :] = mine_ref[0, part, first : first + per, :]
            for k in range(per):
                row = (half - e * per - k) if e * per + k else 0
                ref_out[e, base + per + k : base + per + k + 1, :] = mine_ref[0, part, row : row + 1, :]

    top = lax.broadcasted_iota(jnp.int32, (half, band), 0) == 0
    for t in range(tilts):
        cos_cos = partial_ref[t, :sines, :band]
        cos_sin = partial_ref[t, :sines, band:]
        sin_cos = partial_ref[t, sines:, :band]
        sin_sin = partial_ref[t, sines:, band:]
        low_re = cos_cos + sin_sin
        low_im = sin_cos - cos_sin
        kinds = (
            (cos_cos - sin_sin)[:half],
            jnp.where(top, low_re[half : half + 1], low_re[:half]),
            -(sin_cos + cos_sin)[:half],
            jnp.where(top, low_im[half : half + 1], low_im[:half]),
        )
        for kind, value in enumerate(kinds):
            base = (t * 4 + kind) * per
            for e in range(owners):
                spec_out[e, base : base + per, :] = value[e * per : (e + 1) * per]

    pl.semaphore_wait(barrier, n - 1)

    def copy_of(out, into, send, recv, k):
        dest = lax.rem(me + k, n)
        return pltpu.make_async_remote_copy(
            src_ref=out.at[dest] if out.shape[0] == owners and len(out.shape) == 3 else out,
            dst_ref=into.at[me],
            send_sem=send.at[k],
            recv_sem=recv.at[k],
            device_id={"slab": dest},
            device_id_type=MESH,
        )

    def waiter(out, into, send, recv, k):
        source = lax.rem(me + n - k, n)
        return pltpu.make_async_remote_copy(
            src_ref=out.at[0] if len(out.shape) == 3 else out,
            dst_ref=into.at[source],
            send_sem=send.at[k],
            recv_sem=recv.at[k],
            device_id={"slab": source},
            device_id_type=MESH,
        )

    scatters = ((spec_out, spec_in, spec_send, spec_recv), (ref_out, ref_in, ref_send, ref_recv))
    for group in scatters:
        for k in range(1, n):
            on_owner(lax.rem(me + k, n), lambda: copy_of(*group, k).start())

    def wave(ints):
        angle = (ints & (length - 1)).astype(F32) * (2.0 * math.pi / length)
        return jnp.cos(angle), jnp.sin(angle)

    freq = lax.broadcasted_iota(jnp.int32, (2 * per, band), 1)
    slot = lax.broadcasted_iota(jnp.int32, (n, 2 * per), 1)
    step = lax.broadcasted_iota(jnp.int32, (n, 2 * per), 0) - n // 2
    lower = slot >= per
    place = me * per + jnp.where(lower, slot - per, slot)
    freq_row = jnp.where(lower, jnp.where(place == 0, -half, -place), place)
    col_waves = [wave(freq * (center_ref[t, 1] - win_cols // 2)) for t in range(tilts)]
    row_waves = [wave(freq_row * (center_ref[t, 0] + step)) for t in range(tilts)]

    def contribute():
        spec_in[me] = spec_out[me]
        ref_in[me] = ref_out[me]
        for group in reversed(scatters):
            for k in range(1, n):
                waiter(*group, k).wait_recv()
        total = spec_in[0]
        for e in range(1, n):
            total = total + spec_in[e]
        real_parts, imag_parts, powers = [], [], []
        ref_powers = []
        for t in range(tilts):
            base = t * 4 * per
            spec_re = total[base : base + 2 * per]
            spec_im = total[base + 2 * per : base + 4 * per]
            owned = ref_in[owner_ref[t]]
            ref_re, ref_im = owned[: 2 * per], owned[2 * per :]
            cross_re = spec_re * ref_re + spec_im * ref_im
            cross_im = spec_im * ref_re - spec_re * ref_im
            cos, sin = col_waves[t]
            real_parts.append(cross_re * cos - cross_im * sin)
            imag_parts.append(cross_re * sin + cross_im * cos)
            powers.append(jnp.sum(spec_re * spec_re + spec_im * spec_im, axis=0, keepdims=True))
            ref_powers.append(jnp.sum(ref_re * ref_re + ref_im * ref_im, axis=0, keepdims=True))
        turned = jnp.dot(
            jnp.concatenate(real_parts + imag_parts, axis=0), window_ref[...],
            precision=lax.Precision.HIGHEST, preferred_element_type=F32,
        )
        mid = tilts * 2 * per
        moved_re = turned[:mid, :win_cols] - turned[mid:, win_cols:]
        moved_im = turned[:mid, win_cols:] + turned[mid:, :win_cols]
        for t in range(tilts):
            here = slice(t * 2 * per, (t + 1) * 2 * per)
            cos, sin = row_waves[t]
            left = jnp.concatenate([cos, -sin], axis=1)
            right = jnp.concatenate([moved_re[here], moved_im[here]], axis=0)
            part_out[t * n : (t + 1) * n, :] = jnp.dot(
                left, right, precision=lax.Precision.HIGHEST, preferred_element_type=F32
            )
            part_out[tilts * n + t : tilts * n + t + 1, :] = powers[t]
            part_out[tilts * n + tilts + t : tilts * n + tilts + t + 1, :] = ref_powers[t]
        for k in range(1, n):
            copy_of(part_out, part_in, part_send, part_recv, k).start()
        part_in[me] = part_out[...]

    part_out[tilts * n :, :] = jnp.zeros_like(part_out[tilts * n :, :])
    on_owner(me, contribute)

    for k in range(1, n):
        source = lax.rem(me + n - k, n)
        on_owner(source, lambda: waiter(part_out, part_in, part_send, part_recv, k).wait_recv())
    total = part_in[0]
    for e in range(1, owners):
        total = total + part_in[e]
    total_ref[...] = total
    for t in range(tilts):
        powers = []
        for kind in range(2):
            row = tilts * n + kind * tilts + t
            powers.append(
                jnp.sum(total[row : row + 1], axis=1, keepdims=True) / (band * band) + 1e-06
            )
        scale = band * jnp.sqrt(powers[0] * powers[1])
        corr = total[t * n : (t + 1) * n] / scale
        peak_ref[t] = jnp.max(corr)
        corr_ref[t] = total_ref[pl.ds(t * n + me, 1), :] / scale

    for group in scatters:
        for k in range(1, n):
            on_owner(lax.rem(me + k, n), lambda: copy_of(*group, k).wait_send())

    def drain():
        for k in range(1, n):
            copy_of(part_out, part_in, part_send, part_recv, k).wait_send()

    on_owner(me, drain)


def exchange(n, length, win_cols, center, owner, partial, mine):
    tilts, count, _ = partial.shape
    band = mine.shape[-1]
    per = max(1, band // 2 // n)
    owners = band // 2 // per
    message = tilts * n + 8 * pl.cdiv(2 * tilts, 8)
    smem = pl.BlockSpec(memory_space=pltpu.SMEM)
    vmem = pl.BlockSpec(memory_space=pltpu.VMEM)
    return pl.pallas_call(
        functools.partial(exchange_kernel, n, length),
        out_shape=(
            jax.ShapeDtypeStruct((tilts, 1, win_cols), F32),
            jax.ShapeDtypeStruct((tilts,), F32),
        ),
        in_specs=[smem, smem, vmem, vmem, vmem],
        out_specs=(vmem, smem),
        scratch_shapes=[
            pltpu.VMEM((owners, 4 * per, band), F32),
            pltpu.VMEM((n, 4 * per, band), F32),
            pltpu.VMEM((owners, tilts * 4 * per, band), F32),
            pltpu.VMEM((n, tilts * 4 * per, band), F32),
            pltpu.VMEM((message, win_cols), F32),
            pltpu.VMEM((n, message, win_cols), F32),
            pltpu.VMEM((message, win_cols), F32),
        ]
        + [pltpu.SemaphoreType.DMA((n,))] * 6,
        compiler_params=pltpu.CompilerParams(
            collective_id=0, has_side_effects=True, vmem_limit_bytes=56 * 1024 * 1024
        ),
        name="exchange",
    )(center, owner, partial, mine, jnp.asarray(window_table(length, band, win_cols)))


def solution(mesh):
    n = mesh.shape["slab"]

    def per_device(volume, shift, weight, left, share, center, owner, bands):
        band = bands.shape[-1]
        partial = partial_spectra(shift, weight, left, share, volume, band)
        return exchange(n, volume.shape[-1], band, center, owner, partial, bands)

    placed = (
        P(("grp", "slab"), None, None),
        P("grp", "slab"),
        P("grp", "slab"),
        P("grp", None),
        P("grp", None),
        P("grp", None),
        P("grp"),
        P(("grp", "slab"), None, None, None),
    )
    return jax.shard_map(
        per_device,
        mesh=mesh,
        in_specs=placed,
        out_specs=(P("grp", "slab", None), P("grp")),
        check_vma=False,
    )
```

```python
import functools
import math

import jax
import jax.numpy as jnp
import numpy as np
from jax import lax
from jax.experimental import pallas as pl
from jax.experimental.pallas import tpu as pltpu
from jax.sharding import PartitionSpec as P

MESH = pl.DeviceIdType.MESH
LANES = 128
CHUNK = 256
BF16 = jnp.bfloat16
F32 = jnp.float32


def phases(left, right, length):
    angle = (np.outer(left, right) % length) * (2.0 * math.pi / length)
    return np.cos(angle), np.sin(angle)


def split(values):
    high = values.astype(np.float32).astype(BF16)
    low = (values - high.astype(np.float64)).astype(np.float32).astype(BF16)
    return high, low


def halves(value):
    high = value.astype(BF16)
    return high, (value - high.astype(F32)).astype(BF16)


def row_table(length, band):
    count = band // 2 + 8
    cos, sin = phases(np.arange(count), np.arange(length), length)
    return np.concatenate(split(np.concatenate([cos, sin])))


def col_table(length, band):
    cos, sin = phases(np.arange(length), np.arange(band), length)
    return np.stack(split(np.concatenate([cos, sin], axis=1)))


def window_table(length, band, columns):
    cos, sin = phases(np.arange(band), np.arange(columns), length)
    return np.concatenate([cos, sin], axis=1).astype(np.float32)


def fused_kernel(
    n, center_ref, owner_ref, shift_ref, weight_ref, left_ref, share_ref, mine_ref, window_ref,
    volume_ref, rowt_ref, colt_ref, out_ref,
    vol, rowt, colt, onehot, rows, rolled, summed, stack, proj, sems,
    ref_out, ref_in, spec_out, spec_in, part_out, part_in, peak_out, peak_in,
    ref_send, ref_recv, spec_send, spec_recv, part_send, part_recv, peak_send, peak_recv,
):
    me = lax.axis_index("slab")
    planes, height, width = volume_ref.shape
    tilts = left_ref.shape[0]
    blocks = width // LANES
    chunks = width // CHUNK
    count = rows.shape[2]

    table = pltpu.make_async_copy(rowt_ref, rowt, sems.at[0])
    table.start()
    loads = []
    for z in range(planes):
        for c in range(chunks):
            part = (z, slice(None), pl.ds(c * CHUNK, CHUNK))
            load = pltpu.make_async_copy(volume_ref.at[part], vol.at[part], sems.at[2 + z * chunks + c])
            load.start()
            loads.append(load)
    last_table = pltpu.make_async_copy(colt_ref, colt, sems.at[1])
    last_table.start()

    band = mine_ref.shape[-1]
    length = width
    half = band // 2
    sines = count // 2
    per = max(1, half // n)
    owners = half // per
    win_cols = out_ref.shape[-1]

    def on_owner(device, body):
        if owners == n:
            body()
        else:
            pl.when(device < owners)(body)

    barrier = pltpu.get_barrier_semaphore()
    for k in range(1, n):
        pl.semaphore_signal(
            barrier, inc=1, device_id={"slab": lax.rem(me + k, n)}, device_id_type=MESH
        )

    def sending(source, into, send, recv, k):
        return pltpu.make_async_remote_copy(
            src_ref=source,
            dst_ref=into.at[me],
            send_sem=send.at[k],
            recv_sem=recv.at[k],
            device_id={"slab": lax.rem(me + k, n)},
            device_id_type=MESH,
        )

    def arriving(into, send, recv, k):
        source = lax.rem(me + n - k, n)
        return pltpu.make_async_remote_copy(
            src_ref=into.at[source],
            dst_ref=into.at[source],
            send_sem=send.at[k],
            recv_sem=recv.at[k],
            device_id={"slab": source},
            device_id_type=MESH,
        )

    def scatter(out, into, send, recv, k):
        return sending(out.at[lax.rem(me + k, n)], into, send, recv, k)

    def scatter_all(*group):
        for k in range(1, n):
            on_owner(lax.rem(me + k, n), lambda: scatter(*group, k).start())

    refs = (ref_out, ref_in, ref_send, ref_recv)
    spectra = [
        (spec_out.at[t], spec_in.at[t], spec_send.at[t], spec_recv.at[t]) for t in range(tilts)
    ]

    for e in range(owners):
        for part in range(2):
            base = part * 2 * per
            first = half + e * per
            ref_out[e, base : base + per, :] = mine_ref[0, part, first : first + per, :]
            for k in range(per):
                row = (half - e * per - k) if e * per + k else 0
                ref_out[e, base + per + k : base + per + k + 1, :] = mine_ref[0, part, row : row + 1, :]

    @pl.loop(0, blocks)
    def _(b):
        first = pl.multiple_of(b * LANES, LANES)
        ids = lax.broadcasted_iota(jnp.int32, (LANES, width), 0) + first
        for t in range(tilts):
            hit = jnp.where(ids == left_ref[t : t + 1, :], 1.0, 0.0)
            onehot[t, pl.ds(first, LANES), :] = hit.astype(BF16)

    table.wait()
    for z in range(planes):
        for c in range(chunks):
            loads[z * chunks + c].wait()
            out = jnp.dot(
                rowt[...], vol[z, :, c * CHUNK : (c + 1) * CHUNK], preferred_element_type=F32
            )
            out = out[:count] + out[count:]
            for b in range(CHUNK // LANES):
                rows[z, c * (CHUNK // LANES) + b] = out[:, b * LANES : (b + 1) * LANES]
        if z == 0:
            pl.semaphore_wait(barrier, n - 1)
            scatter_all(*refs)

    lane = lax.broadcasted_iota(jnp.int32, (count, LANES), 1)
    zero = jnp.zeros((count, LANES), F32)
    top = lax.broadcasted_iota(jnp.int32, (half, band), 0) == 0
    for t in range(tilts):
        terms = []
        for z in range(planes):
            for extra in range(2):
                slot = z * 2 + extra
                shift = shift_ref[t, z] + extra
                turn = shift & (LANES - 1)
                jump = jnp.where(shift < 0, 1, 0)
                weight = weight_ref[t, z] if extra else 1.0 - weight_ref[t, z]
                rolled[slot, 0] = zero
                rolled[slot, blocks + 1] = zero
                for b in range(blocks):
                    rolled[slot, b + 1] = pltpu.roll(rows[z, b] * weight, turn, 1)
                terms.append((slot, lane >= turn, jump))
        for b in range(blocks):
            total = None
            for slot, mask, jump in terms:
                term = jnp.where(mask, rolled[slot, b + 1 + jump], rolled[slot, b + jump])
                total = term if total is None else total + term
            summed[b] = total
            high, low = halves(total)
            here = slice(b * LANES, (b + 1) * LANES)
            stack[0, :, here] = high
            stack[1, :, here] = low
        for b in range(blocks):
            ahead = summed[(b + 1) % blocks]
            right = pltpu.roll(jnp.where(lane == 0, ahead, summed[b]), LANES - 1, 1)
            high, low = halves(right)
            here = slice(b * LANES, (b + 1) * LANES)
            stack[2, :, here] = high
            stack[3, :, here] = low
        for c in range(chunks):
            here = slice(c * CHUNK, (c + 1) * CHUNK)
            picked = jnp.dot(
                stack[...].reshape(4 * count, width), onehot[t, :, here], preferred_element_type=F32
            )
            share = share_ref[t : t + 1, here]
            value = (1.0 - share) * (picked[:count] + picked[count : 2 * count])
            value = value + share * (picked[2 * count : 3 * count] + picked[3 * count :])
            high, low = halves(value)
            proj[0, :, here] = high
            proj[1, :, here] = low
        if t == 0:
            last_table.wait()
        both = jnp.dot(
            proj[...].reshape(2 * count, width), colt[0], preferred_element_type=F32
        )
        rest = jnp.dot(proj[0], colt[1], preferred_element_type=F32)
        partial = both[:count] + both[count:] + rest
        cos_cos = partial[:sines, :band]
        cos_sin = partial[:sines, band:]
        sin_cos = partial[sines:, :band]
        sin_sin = partial[sines:, band:]
        low_re = cos_cos + sin_sin
        low_im = sin_cos - cos_sin
        kinds = (
            (cos_cos - sin_sin)[:half],
            jnp.where(top, low_re[half : half + 1], low_re[:half]),
            -(sin_cos + cos_sin)[:half],
            jnp.where(top, low_im[half : half + 1], low_im[:half]),
        )
        for kind, value in enumerate(kinds):
            base = kind * per
            for e in range(owners):
                spec_out[t, e, base : base + per, :] = value[e * per : (e + 1) * per]
        scatter_all(*spectra[t])

    def wave(ints):
        angle = (ints & (length - 1)).astype(F32) * (2.0 * math.pi / length)
        return jnp.cos(angle), jnp.sin(angle)

    freq = lax.broadcasted_iota(jnp.int32, (2 * per, band), 1)
    slot = lax.broadcasted_iota(jnp.int32, (n, 2 * per), 1)
    step = lax.broadcasted_iota(jnp.int32, (n, 2 * per), 0) - n // 2
    lower = slot >= per
    place = me * per + jnp.where(lower, slot - per, slot)
    freq_row = jnp.where(lower, jnp.where(place == 0, -half, -place), place)
    col_waves = [wave(freq * (center_ref[t, 1] - win_cols // 2)) for t in range(tilts)]
    row_waves = [wave(freq_row * (center_ref[t, 0] + step)) for t in range(tilts)]
    spot = lax.broadcasted_iota(jnp.int32, (1, win_cols), 1)

    def contribute():
        ref_in[me] = ref_out[me]
        for k in range(1, n):
            arriving(*refs[1:], k).wait_recv()
        real_parts, imag_parts = [], []
        energy = jnp.zeros((1, win_cols), F32)
        for t in range(tilts):
            spec_in[t, me] = spec_out[t, me]
            for k in range(1, n):
                arriving(*spectra[t][1:], k).wait_recv()
            total = spec_in[t, 0]
            for e in range(1, n):
                total = total + spec_in[t, e]
            spec_re, spec_im = total[: 2 * per], total[2 * per :]
            owned = ref_in[owner_ref[t]]
            ref_re, ref_im = owned[: 2 * per], owned[2 * per :]
            cross_re = spec_re * ref_re + spec_im * ref_im
            cross_im = spec_im * ref_re - spec_re * ref_im
            cos, sin = col_waves[t]
            real_parts.append(cross_re * cos - cross_im * sin)
            imag_parts.append(cross_re * sin + cross_im * cos)
            for kind, (real, imag) in enumerate(((spec_re, spec_im), (ref_re, ref_im))):
                power = jnp.sum(real * real + imag * imag, axis=0, keepdims=True)
                power = jnp.sum(power, axis=1, keepdims=True)
                energy = jnp.where(spot == kind * tilts + t, power, energy)
        turned = jnp.dot(
            jnp.concatenate(real_parts + imag_parts, axis=0), window_ref[...],
            precision=lax.Precision.HIGHEST, preferred_element_type=F32,
        )
        mid = tilts * 2 * per
        moved_re = turned[:mid, :win_cols] - turned[mid:, win_cols:]
        moved_im = turned[:mid, win_cols:] + turned[mid:, :win_cols]
        for t in range(tilts):
            here = slice(t * 2 * per, (t + 1) * 2 * per)
            cos, sin = row_waves[t]
            left = jnp.concatenate([cos, -sin], axis=1)
            right = jnp.concatenate([moved_re[here], moved_im[here]], axis=0)
            value = jnp.dot(
                left, right, precision=lax.Precision.HIGHEST, preferred_element_type=F32
            )
            for i in range(n):
                part_out[i, t : t + 1, :] = value[i : i + 1]
        for i in range(n):
            part_out[i, tilts : tilts + 1, :] = energy
        for k in range(1, n):
            scatter(part_out, part_in, part_send, part_recv, k).start()
        part_in[me] = part_out[me]

    on_owner(me, contribute)

    for k in range(1, n):
        source = lax.rem(me + n - k, n)
        on_owner(source, lambda: arriving(part_in, part_send, part_recv, k).wait_recv())
    total = part_in[0]
    for e in range(1, owners):
        total = total + part_in[e]
    means = total[tilts : tilts + 1] / (band * band) + 1e-06
    lines = []
    for t in range(tilts):
        scale = band * jnp.sqrt(means[:, t : t + 1] * means[:, tilts + t : tilts + t + 1])
        lines.append(total[t : t + 1] / scale)
    line = jnp.concatenate(lines, axis=0)
    peak_out[...] = line
    for k in range(1, n):
        sending(peak_out, peak_in, peak_send, peak_recv, k).start()
    peak_in[me] = line
    out_ref[0] = line
    for group in [refs] + spectra:
        for k in range(1, n):
            on_owner(lax.rem(me + k, n), lambda: scatter(*group, k).wait_send())

    def drain():
        for k in range(1, n):
            scatter(part_out, part_in, part_send, part_recv, k).wait_send()

    on_owner(me, drain)
    for k in range(1, n):
        arriving(peak_in, peak_send, peak_recv, k).wait_recv()
    best = peak_in[0]
    for e in range(1, n):
        best = jnp.maximum(best, peak_in[e])
    out_ref[1] = best
    for k in range(1, n):
        sending(peak_out, peak_in, peak_send, peak_recv, k).wait_send()


def finish_kernel(both_ref, corr_ref, peak_ref):
    for t in range(both_ref.shape[1]):
        corr_ref[t] = both_ref[0, t : t + 1, :]
        peak_ref[t] = jnp.max(both_ref[1, t : t + 1, :])


def run(n, volume, shift, weight, left, share, center, owner, mine):
    planes, height, width = volume.shape
    tilts = left.shape[0]
    band = mine.shape[-1]
    win_cols = band
    rowt = row_table(height, band)
    colt = col_table(width, band)
    window = window_table(width, band, win_cols)
    count = rowt.shape[0] // 2
    blocks = width // LANES
    per = max(1, band // 2 // n)
    owners = band // 2 // per
    smem = pl.BlockSpec(memory_space=pltpu.SMEM)
    vmem = pl.BlockSpec(memory_space=pltpu.VMEM)
    hbm = pl.BlockSpec(memory_space=pl.ANY)
    dma = pltpu.SemaphoreType.DMA
    both = pl.pallas_call(
        functools.partial(fused_kernel, n),
        out_shape=jax.ShapeDtypeStruct((2, tilts, win_cols), F32),
        in_specs=[smem] * 4 + [vmem] * 4 + [hbm] * 3,
        out_specs=vmem,
        scratch_shapes=[
            pltpu.VMEM((planes, height, width), BF16),
            pltpu.VMEM(rowt.shape, BF16),
            pltpu.VMEM(colt.shape, BF16),
            pltpu.VMEM((tilts, width, width), BF16),
            pltpu.VMEM((planes, blocks, count, LANES), F32),
            pltpu.VMEM((planes * 2, blocks + 2, count, LANES), F32),
            pltpu.VMEM((blocks, count, LANES), F32),
            pltpu.VMEM((4, count, width), BF16),
            pltpu.VMEM((2, count, width), BF16),
            dma((2 + planes * (width // CHUNK),)),
            pltpu.VMEM((owners, 4 * per, band), F32),
            pltpu.VMEM((n, 4 * per, band), F32),
            pltpu.VMEM((tilts, owners, 4 * per, band), F32),
            pltpu.VMEM((tilts, n, 4 * per, band), F32),
            pltpu.VMEM((n, tilts + 1, win_cols), F32),
            pltpu.VMEM((n, tilts + 1, win_cols), F32),
            pltpu.VMEM((tilts, win_cols), F32),
            pltpu.VMEM((n, tilts, win_cols), F32),
            dma((n,)), dma((n,)), dma((tilts, n)), dma((tilts, n)),
            dma((n,)), dma((n,)), dma((n,)), dma((n,)),
        ],
        compiler_params=pltpu.CompilerParams(
            collective_id=0, has_side_effects=True, vmem_limit_bytes=56 * 1024 * 1024
        ),
        name="fused",
    )(
        center, owner, shift, weight, left, share, mine, jnp.asarray(window),
        volume, jnp.asarray(rowt), jnp.asarray(colt),
    )
    return pl.pallas_call(
        finish_kernel,
        out_shape=(
            jax.ShapeDtypeStruct((tilts, 1, win_cols), F32),
            jax.ShapeDtypeStruct((tilts,), F32),
        ),
        in_specs=[vmem],
        out_specs=(vmem, smem),
        name="finish",
    )(both)


def solution(mesh):
    n = mesh.shape["slab"]

    def per_device(volume, shift, weight, left, share, center, owner, bands):
        return run(n, volume, shift, weight, left, share, center, owner, bands)

    placed = (
        P(("grp", "slab"), None, None),
        P("grp", "slab"),
        P("grp", "slab"),
        P("grp", None),
        P("grp", None),
        P("grp", None),
        P("grp"),
        P(("grp", "slab"), None, None, None),
    )
    return jax.shard_map(
        per_device,
        mesh=mesh,
        in_specs=placed,
        out_specs=(P("grp", "slab", None), P("grp")),
        check_vma=False,
    )
```

```python
import functools
import math

import jax
import jax.numpy as jnp
import numpy as np
from jax import lax
from jax.experimental import pallas as pl
from jax.experimental.pallas import tpu as pltpu
from jax.sharding import PartitionSpec as P

MESH = pl.DeviceIdType.MESH
LANES = 128
CHUNK = 256
BF16 = jnp.bfloat16
F32 = jnp.float32


def phases(left, right, length):
    angle = (np.outer(left, right) % length) * (2.0 * math.pi / length)
    return np.cos(angle), np.sin(angle)


def split(values):
    high = values.astype(np.float32).astype(BF16)
    low = (values - high.astype(np.float64)).astype(np.float32).astype(BF16)
    return high, low


def halves(value):
    high = value.astype(BF16)
    return high, (value - high.astype(F32)).astype(BF16)


def product(first, second):
    count = first[0].shape[0]
    both = jnp.dot(jnp.concatenate(first, axis=0), second[0], preferred_element_type=F32)
    rest = jnp.dot(first[0], second[1], preferred_element_type=F32)
    return both[:count] + both[count:] + rest


def row_table(length, band):
    count = band // 2 + 8
    cos, sin = phases(np.arange(count), np.arange(length), length)
    return np.concatenate(split(np.concatenate([cos, sin])))


def col_table(length, band):
    cos, sin = phases(np.arange(length), np.arange(band), length)
    return np.stack(split(np.concatenate([cos, sin], axis=1)))


def window_table(length, band, columns):
    cos, sin = phases(np.arange(band), np.arange(columns), length)
    return np.stack(split(np.concatenate([cos, sin], axis=1)))


def fused_kernel(
    n, center_ref, owner_ref, shift_ref, weight_ref, left_ref, share_ref, mine_ref, window_ref,
    volume_ref, rowt_ref, colt_ref, out_ref,
    vol, rowt, colt, mine_vmem, window_vmem, onehot, rolled, summed, stack, proj, sems,
    ref_out, ref_in, spec_out, spec_in, part_out, part_in, peak_out, peak_in,
    ref_send, ref_recv, spec_send, spec_recv, part_send, part_recv, peak_send, peak_recv,
):
    me = lax.axis_index("slab")
    planes, height, width = volume_ref.shape
    tilts = left_ref.shape[0]
    blocks = width // LANES
    chunks = width // CHUNK
    count = rowt.shape[0] // 2

    table = pltpu.make_async_copy(rowt_ref, rowt, sems.at[0])
    table.start()
    loads = []
    for z in range(planes):
        for c in range(chunks):
            part = (z, slice(None), pl.ds(c * CHUNK, CHUNK))
            load = pltpu.make_async_copy(volume_ref.at[part], vol.at[part], sems.at[4 + z * chunks + c])
            load.start()
            loads.append(load)
    last_table = pltpu.make_async_copy(colt_ref, colt, sems.at[1])
    last_table.start()
    mine_copy = pltpu.make_async_copy(mine_ref, mine_vmem, sems.at[2])
    mine_copy.start()
    window_copy = pltpu.make_async_copy(window_ref, window_vmem, sems.at[3])
    window_copy.start()

    band = mine_ref.shape[-1]
    length = width
    half = band // 2
    sines = count // 2
    per = max(1, half // n)
    owners = half // per
    win_cols = out_ref.shape[-1]

    def on_owner(device, body):
        if owners == n:
            body()
        else:
            pl.when(device < owners)(body)

    barrier = pltpu.get_barrier_semaphore()
    for k in range(1, n):
        pl.semaphore_signal(
            barrier, inc=1, device_id={"slab": lax.rem(me + k, n)}, device_id_type=MESH
        )

    def sending(source, into, send, recv, k):
        return pltpu.make_async_remote_copy(
            src_ref=source,
            dst_ref=into.at[me],
            send_sem=send.at[k],
            recv_sem=recv.at[k],
            device_id={"slab": lax.rem(me + k, n)},
            device_id_type=MESH,
        )

    def arriving(into, send, recv, k):
        source = lax.rem(me + n - k, n)
        return pltpu.make_async_remote_copy(
            src_ref=into.at[source],
            dst_ref=into.at[source],
            send_sem=send.at[k],
            recv_sem=recv.at[k],
            device_id={"slab": source},
            device_id_type=MESH,
        )

    def scatter(out, into, send, recv, k):
        return sending(out.at[lax.rem(me + k, n)], into, send, recv, k)

    def scatter_all(*group):
        for k in range(1, n):
            on_owner(lax.rem(me + k, n), lambda: scatter(*group, k).start())

    refs = (ref_out, ref_in, ref_send, ref_recv)
    spectra = [
        (spec_out.at[t], spec_in.at[t], spec_send.at[t], spec_recv.at[t]) for t in range(tilts)
    ]

    def order_refs():
        for e in range(owners):
            for part in range(2):
                base = part * 2 * per
                first = half + e * per
                ref_out[e, base : base + per, :] = mine_vmem[0, part, first : first + per, :]
                for k in range(per):
                    row = (half - e * per - k) if e * per + k else 0
                    ref_out[e, base + per + k : base + per + k + 1, :] = mine_vmem[0, part, row : row + 1, :]

    @pl.loop(0, blocks)
    def _(b):
        first = pl.multiple_of(b * LANES, LANES)
        ids = lax.broadcasted_iota(jnp.int32, (LANES, width), 0) + first
        for t in range(tilts):
            hit = jnp.where(ids == left_ref[t : t + 1, :], 1.0, 0.0)
            onehot[t, pl.ds(first, LANES), :] = hit.astype(BF16)

    lane = lax.broadcasted_iota(jnp.int32, (count, LANES), 1)
    zero = jnp.zeros((count, LANES), F32)
    top = lax.broadcasted_iota(jnp.int32, (half, band), 0) == 0
    turns, jumps, weights = [], [], []
    for t in range(tilts):
        shifts = [shift_ref[t, z] for z in range(planes)]
        turns.append([shift & (LANES - 1) for shift in shifts])
        jumps.append([jnp.where(shift < 0, 1, 0) for shift in shifts])
        weights.append([weight_ref[t, z] for z in range(planes)])
        for z in range(planes):
            rolled[t, z, 0] = zero
            rolled[t, z, 1] = zero
            rolled[t, z, blocks + 2] = zero

    table.wait()
    for z in range(planes):
        for c in range(chunks):
            loads[z * chunks + c].wait()
            out = jnp.dot(
                rowt[...], vol[z, :, c * CHUNK : (c + 1) * CHUNK], preferred_element_type=F32
            )
            out = out[:count] + out[count:]
            for b in range(CHUNK // LANES):
                block = out[:, b * LANES : (b + 1) * LANES]
                for t in range(tilts):
                    rolled[t, z, c * (CHUNK // LANES) + b + 2] = pltpu.roll(block, turns[t][z], 1)
        if z == 0:
            mine_copy.wait()
            order_refs()
            pl.semaphore_wait(barrier, n - 1)
            scatter_all(*refs)

    def combine(t, b):
        near, far = zero, zero
        for z in range(planes):
            jump = jumps[t][z]
            if b < 0:
                value = rolled[t, z, b + 2 + jump]
            else:
                value = jnp.where(
                    lane >= turns[t][z], rolled[t, z, b + 2 + jump], rolled[t, z, b + 1 + jump]
                )
            near = near + (1.0 - weights[t][z]) * value
            far = far + weights[t][z] * value
        summed[t, 0, b + 1] = near
        summed[t, 1, b + 1] = far

    def place_block(t, b):
        near, far = summed[t, 0, b + 1], summed[t, 1, b + 1]
        ahead = summed[t, 0, (b + 1) % blocks + 1]
        behind = summed[t, 1, b]
        left = near + pltpu.roll(jnp.where(lane == LANES - 1, behind, far), 1, 1)
        right = far + pltpu.roll(jnp.where(lane == 0, ahead, near), LANES - 1, 1)
        here = slice(b * LANES, (b + 1) * LANES)
        for slot, value in enumerate(halves(left) + halves(right)):
            stack[t, slot, :, here] = value

    def tasks(t):
        made = [functools.partial(combine, t, b) for b in range(-1, blocks)]
        return made + [functools.partial(place_block, t, b) for b in range(blocks)]

    for task in tasks(0):
        task()
    for t in range(tilts):
        later = tasks(t + 1) if t + 1 < tilts else []
        share_of = -(-len(later) // chunks)
        for c in range(chunks):
            here = slice(c * CHUNK, (c + 1) * CHUNK)
            picked = jnp.dot(
                stack[t].reshape(4 * count, width), onehot[t, :, here], preferred_element_type=F32
            )
            share = share_ref[t : t + 1, here]
            value = (1.0 - share) * (picked[:count] + picked[count : 2 * count])
            value = value + share * (picked[2 * count : 3 * count] + picked[3 * count :])
            high, low = halves(value)
            proj[t, 0, :, here] = high
            proj[t, 1, :, here] = low
            for task in later[c * share_of : (c + 1) * share_of]:
                task()
        if t == 0:
            last_table.wait()
        both = jnp.dot(
            proj[t].reshape(2 * count, width), colt[0], preferred_element_type=F32
        )
        rest = jnp.dot(proj[t, 0], colt[1], preferred_element_type=F32)
        partial = both[:count] + both[count:] + rest
        cos_cos = partial[:sines, :band]
        cos_sin = partial[:sines, band:]
        sin_cos = partial[sines:, :band]
        sin_sin = partial[sines:, band:]
        low_re = cos_cos + sin_sin
        low_im = sin_cos - cos_sin
        kinds = (
            (cos_cos - sin_sin)[:half],
            jnp.where(top, low_re[half : half + 1], low_re[:half]),
            -(sin_cos + cos_sin)[:half],
            jnp.where(top, low_im[half : half + 1], low_im[:half]),
        )
        for kind, value in enumerate(kinds):
            base = kind * per
            for e in range(owners):
                spec_out[t, e, base : base + per, :] = value[e * per : (e + 1) * per]
        scatter_all(*spectra[t])

    def wave(ints):
        angle = (ints & (length - 1)).astype(F32) * (2.0 * math.pi / length)
        return jnp.cos(angle), jnp.sin(angle)

    freq = lax.broadcasted_iota(jnp.int32, (2 * per, band), 1)
    slot = lax.broadcasted_iota(jnp.int32, (n, 2 * per), 1)
    step = lax.broadcasted_iota(jnp.int32, (n, 2 * per), 0) - n // 2
    lower = slot >= per
    place = me * per + jnp.where(lower, slot - per, slot)
    freq_row = jnp.where(lower, jnp.where(place == 0, -half, -place), place)
    col_waves = [wave(freq * (center_ref[t, 1] - win_cols // 2)) for t in range(tilts)]
    row_waves = []
    for t in range(tilts):
        cos, sin = wave(freq_row * (center_ref[t, 0] + step))
        row_waves.append(halves(jnp.concatenate([cos, -sin], axis=1)))
    window_copy.wait()
    spot = lax.broadcasted_iota(jnp.int32, (1, win_cols), 1)

    def contribute():
        ref_in[me] = ref_out[me]
        for k in range(1, n):
            arriving(*refs[1:], k).wait_recv()
        real_parts, imag_parts = [], []
        energy = jnp.zeros((1, win_cols), F32)
        for t in range(tilts):
            spec_in[t, me] = spec_out[t, me]
            for k in range(1, n):
                arriving(*spectra[t][1:], k).wait_recv()
            total = spec_in[t, 0]
            for e in range(1, n):
                total = total + spec_in[t, e]
            spec_re, spec_im = total[: 2 * per], total[2 * per :]
            owned = ref_in[owner_ref[t]]
            ref_re, ref_im = owned[: 2 * per], owned[2 * per :]
            cross_re = spec_re * ref_re + spec_im * ref_im
            cross_im = spec_im * ref_re - spec_re * ref_im
            cos, sin = col_waves[t]
            real_parts.append(cross_re * cos - cross_im * sin)
            imag_parts.append(cross_re * sin + cross_im * cos)
            for kind, (real, imag) in enumerate(((spec_re, spec_im), (ref_re, ref_im))):
                power = jnp.sum(real * real + imag * imag, axis=0, keepdims=True)
                power = jnp.sum(power, axis=1, keepdims=True)
                energy = jnp.where(spot == kind * tilts + t, power, energy)
        turned = product(
            halves(jnp.concatenate(real_parts + imag_parts, axis=0)),
            (window_vmem[0], window_vmem[1]),
        )
        mid = tilts * 2 * per
        moved_re = turned[:mid, :win_cols] - turned[mid:, win_cols:]
        moved_im = turned[:mid, win_cols:] + turned[mid:, :win_cols]
        for t in range(tilts):
            here = slice(t * 2 * per, (t + 1) * 2 * per)
            right = jnp.concatenate([moved_re[here], moved_im[here]], axis=0)
            value = product(row_waves[t], halves(right))
            for i in range(n):
                part_out[i, t : t + 1, :] = value[i : i + 1]
        for i in range(n):
            part_out[i, tilts : tilts + 1, :] = energy
        for k in range(1, n):
            scatter(part_out, part_in, part_send, part_recv, k).start()
        part_in[me] = part_out[me]

    on_owner(me, contribute)

    for k in range(1, n):
        source = lax.rem(me + n - k, n)
        on_owner(source, lambda: arriving(part_in, part_send, part_recv, k).wait_recv())
    total = part_in[0]
    for e in range(1, owners):
        total = total + part_in[e]
    means = total[tilts : tilts + 1] / (band * band) + 1e-06
    lines = []
    for t in range(tilts):
        scale = band * jnp.sqrt(means[:, t : t + 1] * means[:, tilts + t : tilts + t + 1])
        lines.append(total[t : t + 1] / scale)
    line = jnp.concatenate(lines, axis=0)
    peak_out[...] = line
    for k in range(1, n):
        sending(peak_out, peak_in, peak_send, peak_recv, k).start()
    peak_in[me] = line
    out_ref[0] = line
    for group in [refs] + spectra:
        for k in range(1, n):
            on_owner(lax.rem(me + k, n), lambda: scatter(*group, k).wait_send())

    def drain():
        for k in range(1, n):
            scatter(part_out, part_in, part_send, part_recv, k).wait_send()

    on_owner(me, drain)
    for k in range(1, n):
        arriving(peak_in, peak_send, peak_recv, k).wait_recv()
    best = peak_in[0]
    for e in range(1, n):
        best = jnp.maximum(best, peak_in[e])
    out_ref[1] = best
    for k in range(1, n):
        sending(peak_out, peak_in, peak_send, peak_recv, k).wait_send()


def finish_kernel(both_ref, corr_ref, peak_ref):
    for t in range(both_ref.shape[1]):
        corr_ref[t] = both_ref[0, t : t + 1, :]
        peak_ref[t] = jnp.max(both_ref[1, t : t + 1, :])


def run(n, volume, shift, weight, left, share, center, owner, mine):
    planes, height, width = volume.shape
    tilts = left.shape[0]
    band = mine.shape[-1]
    win_cols = band
    rowt = row_table(height, band)
    colt = col_table(width, band)
    window = window_table(width, band, win_cols)
    count = rowt.shape[0] // 2
    blocks = width // LANES
    per = max(1, band // 2 // n)
    owners = band // 2 // per
    smem = pl.BlockSpec(memory_space=pltpu.SMEM)
    vmem = pl.BlockSpec(memory_space=pltpu.VMEM)
    hbm = pl.BlockSpec(memory_space=pl.ANY)
    dma = pltpu.SemaphoreType.DMA
    both = pl.pallas_call(
        functools.partial(fused_kernel, n),
        out_shape=jax.ShapeDtypeStruct((2, tilts, win_cols), F32),
        in_specs=[smem] * 4 + [vmem] * 2 + [hbm] * 5,
        out_specs=vmem,
        scratch_shapes=[
            pltpu.VMEM((planes, height, width), BF16),
            pltpu.VMEM(rowt.shape, BF16),
            pltpu.VMEM(colt.shape, BF16),
            pltpu.VMEM(mine.shape, F32),
            pltpu.VMEM(window.shape, BF16),
            pltpu.VMEM((tilts, width, width), BF16),
            pltpu.VMEM((tilts, planes, blocks + 3, count, LANES), F32),
            pltpu.VMEM((tilts, 2, blocks + 1, count, LANES), F32),
            pltpu.VMEM((tilts, 4, count, width), BF16),
            pltpu.VMEM((tilts, 2, count, width), BF16),
            dma((4 + planes * (width // CHUNK),)),
            pltpu.VMEM((owners, 4 * per, band), F32),
            pltpu.VMEM((n, 4 * per, band), F32),
            pltpu.VMEM((tilts, owners, 4 * per, band), F32),
            pltpu.VMEM((tilts, n, 4 * per, band), F32),
            pltpu.VMEM((n, tilts + 1, win_cols), F32),
            pltpu.VMEM((n, tilts + 1, win_cols), F32),
            pltpu.VMEM((tilts, win_cols), F32),
            pltpu.VMEM((n, tilts, win_cols), F32),
            dma((n,)), dma((n,)), dma((tilts, n)), dma((tilts, n)),
            dma((n,)), dma((n,)), dma((n,)), dma((n,)),
        ],
        compiler_params=pltpu.CompilerParams(
            collective_id=0, has_side_effects=True, vmem_limit_bytes=56 * 1024 * 1024
        ),
        name="fused",
    )(
        center, owner, shift, weight, left, share, mine, jnp.asarray(window),
        volume, jnp.asarray(rowt), jnp.asarray(colt),
    )
    return pl.pallas_call(
        finish_kernel,
        out_shape=(
            jax.ShapeDtypeStruct((tilts, 1, win_cols), F32),
            jax.ShapeDtypeStruct((tilts,), F32),
        ),
        in_specs=[vmem],
        out_specs=(vmem, smem),
        name="finish",
    )(both)


def solution(mesh):
    n = mesh.shape["slab"]

    def per_device(volume, shift, weight, left, share, center, owner, bands):
        return run(n, volume, shift, weight, left, share, center, owner, bands)

    placed = (
        P(("grp", "slab"), None, None),
        P("grp", "slab"),
        P("grp", "slab"),
        P("grp", None),
        P("grp", None),
        P("grp", None),
        P("grp"),
        P(("grp", "slab"), None, None, None),
    )
    return jax.shard_map(
        per_device,
        mesh=mesh,
        in_specs=placed,
        out_specs=(P("grp", "slab", None), P("grp")),
        check_vma=False,
    )
```
